16 devices in a mesh: fsdp: 16 (over z, y, x, core).
Axes of the slice: x: 2, y: 2, z: 2, core: 2. Of those that a mesh axis runs over, the one named last changes fastest.
Arguments:
- h_in: bfloat16 [32, 1024, 1024], P('fsdp')
- w_gate: bfloat16 [4, 1024, 3072], P(None, 'fsdp')
- w_up: bfloat16 [4, 1024, 3072], P(None, 'fsdp')
- w_down: bfloat16 [4, 3072, 1024], P(None, 'fsdp')
- grad_out: bfloat16 [32, 1024, 1024], P('fsdp')
Outputs:
- output 1: bfloat16 [32, 1024, 1024], P('fsdp')
- output 2: bfloat16 [32, 1024, 1024], P('fsdp')
- output 3: float32 [4, 1024, 3072], P(None, 'fsdp')
- output 4: float32 [4, 1024, 3072], P(None, 'fsdp')
- output 5: float32 [4, 3072, 1024], P(None, 'fsdp')
All inputs are finite; a program needn't handle non-finite values.
Results may differ from the reference program's by a relative error of at most 0.0164932.
Values are sent between devices in bfloat16 or wider.
A program may use at most 1 GiB of HBM per device.

```python
import jax
import jax.numpy as jnp
from jax import lax

BATCH = 32
SEQ = 1024
D = 1024
FF = 3072
LAYERS = 4
NORM_EPS = 1e-5


def setup_inputs(seed: int = 0) -> dict:
    key_list = jax.random.split(jax.random.key(seed), 5)
    h_in = jax.random.normal(key_list[0], (BATCH, SEQ, D), jnp.float32).astype(jnp.bfloat16)
    w_gate = (jax.random.normal(key_list[1], (LAYERS, D, FF), jnp.float32) * D ** -0.5).astype(jnp.bfloat16)
    w_up = (jax.random.normal(key_list[2], (LAYERS, D, FF), jnp.float32) * D ** -0.5).astype(jnp.bfloat16)
    w_down = (jax.random.normal(key_list[3], (LAYERS, FF, D), jnp.float32) * FF ** -0.5).astype(jnp.bfloat16)
    grad_out = jax.random.normal(key_list[4], (BATCH, SEQ, D), jnp.float32).astype(jnp.bfloat16)
    return {"h_in": h_in, "w_gate": w_gate, "w_up": w_up, "w_down": w_down, "grad_out": grad_out}


def rms_parts(h_row):
    h_f32 = h_row.astype(jnp.float32)
    inv_rms = lax.rsqrt(jnp.mean(h_f32 * h_f32, axis=-1, keepdims=True) + NORM_EPS)
    return h_f32, inv_rms, (h_f32 * inv_rms).astype(jnp.bfloat16)


def block_fwd(h_row, gate_wt, up_wt, down_wt):
    h_f32, inv_rms, normed = rms_parts(h_row)
    gate_pre = jnp.dot(normed, gate_wt, preferred_element_type=jnp.float32)
    up_pre = jnp.dot(normed, up_wt, preferred_element_type=jnp.float32)
    act_out = (gate_pre * jax.nn.sigmoid(gate_pre) * up_pre).astype(jnp.bfloat16)
    return (h_f32 + jnp.dot(act_out, down_wt, preferred_element_type=jnp.float32)).astype(jnp.bfloat16)


def block_bwd(h_row, g_row, gate_wt, up_wt, down_wt):
    h_f32, inv_rms, normed = rms_parts(h_row)
    gate_pre = jnp.dot(normed, gate_wt, preferred_element_type=jnp.float32)
    up_pre = jnp.dot(normed, up_wt, preferred_element_type=jnp.float32)
    sig_gate = jax.nn.sigmoid(gate_pre)
    silu_gate = gate_pre * sig_gate
    act_out = (silu_gate * up_pre).astype(jnp.bfloat16)
    d_act = jnp.dot(g_row, down_wt.T, preferred_element_type=jnp.float32)
    d_gate = (d_act * up_pre * (sig_gate * (1.0 + gate_pre * (1.0 - sig_gate)))).astype(jnp.bfloat16)
    d_up = (d_act * silu_gate).astype(jnp.bfloat16)
    d_norm = jnp.dot(d_gate, gate_wt.T, preferred_element_type=jnp.float32) + jnp.dot(d_up, up_wt.T, preferred_element_type=jnp.float32)
    d_hid = inv_rms * d_norm - h_f32 * (inv_rms * inv_rms * inv_rms) * jnp.mean(d_norm * h_f32, axis=-1, keepdims=True)
    new_grad = (g_row.astype(jnp.float32) + d_hid).astype(jnp.bfloat16)
    row_grads = (
        jnp.dot(normed.T, d_gate, preferred_element_type=jnp.float32),
        jnp.dot(normed.T, d_up, preferred_element_type=jnp.float32),
        jnp.dot(act_out.T, g_row, preferred_element_type=jnp.float32),
    )
    return new_grad, row_grads


def reference(h_in, w_gate, w_up, w_down, grad_out):
    def fwd_layer(hidden, weights):
        gate_wt, up_wt, down_wt = weights
        h_next = lax.map(lambda h_row: block_fwd(h_row, gate_wt, up_wt, down_wt), hidden)
        return h_next, hidden

    h_out, saved_h = lax.scan(fwd_layer, h_in, (w_gate, w_up, w_down))

    def bwd_layer(grad_in, inputs):
        hidden, gate_wt, up_wt, down_wt = inputs

        def row_step(acc_grads, row_pair):
            h_row, g_row = row_pair
            new_row, row_grads = block_bwd(h_row, g_row, gate_wt, up_wt, down_wt)
            return tuple(acc_part + row_part for acc_part, row_part in zip(acc_grads, row_grads)), new_row

        zero_acc = (jnp.zeros((D, FF), jnp.float32), jnp.zeros((D, FF), jnp.float32), jnp.zeros((FF, D), jnp.float32))
        grad_sums, new_grad = lax.scan(row_step, zero_acc, (hidden, grad_in))
        return new_grad, grad_sums

    dh_in, layer_grads = lax.scan(bwd_layer, grad_out, (saved_h, w_gate, w_up, w_down), reverse=True)
    return h_out, dh_in, layer_grads[0], layer_grads[1], layer_grads[2]
```

```python
import functools

import jax
import jax.numpy as jnp
from jax import lax
from jax.experimental import pallas as pl
from jax.experimental.pallas import tpu as pltpu
from jax.sharding import PartitionSpec as P


NORM_EPS = 1e-5
CORE, X, Y, Z = 1, 2, 4, 8
AXIS_BITS = (X, Y, Z)
TM = 1024
TF = 768
SUB_FWD, SUB_BWD = 2, 4
TD = 512
VMEM_BYTES = 60 * 1024 * 1024
FLIGHT, T_DOWN, T_BWD, T_IN = 95.0, 21.0, 66.0, 20.0


def params(semantics):
    return pltpu.CompilerParams(dimension_semantics=semantics, vmem_limit_bytes=VMEM_BYTES)


def t_dot(lhs, rhs):
    return lax.dot_general(lhs, rhs, (((0,), (0,)), ((), ())), preferred_element_type=jnp.float32)


MESH_ID = pl.DeviceIdType.MESH
GATHER_STEPS = (0, 2, 5, 7)


class Gather:
    def __init__(self, axis, shards, fulls, sends, recvs, locals_):
        self.shards, self.fulls = shards, fulls
        self.sends, self.recvs, self.locals_ = sends, recvs, locals_
        me = lax.axis_index(axis)
        self.core = me % 2
        self.coord = {Z: me // 8, Y: (me // 4) % 2, X: (me // 2) % 2}
        self.partner = {
            CORE: me + 1 - 2 * self.core,
            X: me + 2 - 4 * self.coord[X],
            Y: me + 4 - 8 * self.coord[Y],
            Z: me + 8 - 16 * self.coord[Z],
        }

    def order(self, k):
        return tuple(AXIS_BITS[(k + i) % 3] for i in range(3))

    def piece(self, k, free=(), flipped=None):
        index = []
        for bit in (Z, Y, X):
            if bit in free:
                index.append(slice(None))
            elif bit == flipped:
                index.append(1 - self.coord[bit])
            else:
                index.append(self.coord[bit])
        return self.fulls[k].at[tuple(index) + (self.core,)]

    def remote(self, k, slot, src, dst, bit):
        return pltpu.make_async_remote_copy(
            src_ref=src,
            dst_ref=dst,
            send_sem=self.sends.at[k, slot],
            recv_sem=self.recvs.at[k, slot],
            device_id=(self.partner[bit],),
            device_id_type=MESH_ID,
        )

    def along(self, k, s, j):
        if j == 0:
            return self.remote(k, (0, 1, 3)[s], self.shards[k], self.piece(k), self.order(k)[s])
        part = self.piece(k, self.order(k)[: j - 1], self.order(k)[j - 1])
        return self.remote(k, (0, 1, 3)[s] + j, part, part, self.order(k)[s])

    def arrived(self, k, s, j):
        return self.along(k, s, j)

    def across(self, k, s, j):
        if s < 0:
            return self.remote(k, 6, self.shards[k], self.piece(k), CORE)
        order = self.order(k)
        free = order[: j - 1] if j > 0 else ()
        index = []
        for bit in (Z, Y, X):
            if bit in free:
                index.append(slice(None))
            elif bit == order[s] or (j > 0 and bit == order[j - 1]):
                index.append(1 - self.coord[bit])
            else:
                index.append(self.coord[bit])
        part = self.fulls[k].at[tuple(index) + (self.core,)]
        return self.remote(k, 7 + (0, 1, 3)[s] + j, part, part, CORE)

    def own(self, k):
        return pltpu.make_async_copy(self.shards[k], self.piece(k), self.locals_.at[k])

    def begin(self):
        barrier = pltpu.get_barrier_semaphore()
        for bit in (CORE, X, Y, Z):
            pl.semaphore_signal(barrier, inc=1, device_id=(self.partner[bit],), device_id_type=MESH_ID)
        pl.semaphore_wait(barrier, 4)
        for s in range(3):
            for k in range(3):
                self.along(k, s, 0).start()
        for k in range(3):
            self.across(k, -1, 0).start()
            self.own(k).start()

    def take(self, k, s, j):
        self.arrived(k, s, j).wait_recv()
        self.across(k, s, j).start()

    def advance(self, s):
        for k in range(3):
            if s == 1:
                self.take(k, 0, 0)
                self.along(k, 1, 1).start()
                self.along(k, 2, 1).start()
            elif s == 2:
                self.take(k, 1, 0)
                self.take(k, 1, 1)
                self.along(k, 2, 2).start()
            else:
                self.take(k, 2, 0)
                self.take(k, 2, 1)

    def finish(self):
        for k in range(3):
            self.take(k, 2, 2)
        for k in range(3):
            self.own(k).wait()
            for s in range(3):
                for j in range(s + 1):
                    self.along(k, s, j).wait_send()
                    self.across(k, s, j).wait()
            self.across(k, -1, 0).wait()


GATHER_SCRATCH = [
    pltpu.SemaphoreType.DMA((3, 13)),
    pltpu.SemaphoreType.DMA((3, 13)),
    pltpu.SemaphoreType.DMA((3,)),
]
ANY = pl.BlockSpec(memory_space=pl.ANY)


def full_shapes(shards):
    return [jax.ShapeDtypeStruct((2, 2, 2, 2) + w.shape, w.dtype) for w in shards]


def flat(fulls):
    return tuple(w.reshape(-1, w.shape[-1]) for w in fulls)


def gather_first(axis, shards):
    def kernel(*refs):
        gather = Gather(axis, refs[:3], refs[3:6], *refs[6:9])
        gather.begin()
        for s in (1, 2, 3):
            gather.advance(s)
        gather.finish()

    return flat(
        pl.pallas_call(
            kernel,
            in_specs=[ANY] * 3,
            out_specs=[ANY] * 3,
            out_shape=full_shapes(shards),
            scratch_shapes=GATHER_SCRATCH,
            compiler_params=pltpu.CompilerParams(collective_id=0, has_side_effects=True),
            name="gather_first",
        )(*shards)
    )


def fwd_gather_kernel(axis, *refs):
    main, shards, outs, fulls, scratch, sems = refs[:4], refs[4:7], refs[7:12], refs[12:15], refs[15:17], refs[17:]
    step = pl.program_id(0) * pl.num_programs(1) + pl.program_id(1)
    gather = Gather(axis, shards, fulls, *sems)
    pl.when(step == GATHER_STEPS[0])(gather.begin)
    for s in (1, 2, 3):
        pl.when(step == GATHER_STEPS[s])(functools.partial(gather.advance, s))
    fwd_kernel(*main, *outs, *scratch)
    pl.when(step == pl.num_programs(0) * pl.num_programs(1) - 1)(gather.finish)


def fwd_kernel(h_ref, wg_ref, wu_ref, wd_ref, out_ref, n_ref, gate_ref, up_ref, act_ref, n_all, acc):
    f, m = pl.program_id(0), pl.program_id(1)
    rows = pl.ds(pl.multiple_of(m * TM, TM), TM)

    @pl.when(f == 0)
    def _():
        h_f32 = h_ref[...].astype(jnp.float32)
        inv_rms = lax.rsqrt(jnp.mean(h_f32 * h_f32, axis=-1, keepdims=True) + NORM_EPS)
        normed = (h_f32 * inv_rms).astype(jnp.bfloat16)
        n_all[rows, :] = normed
        n_ref[...] = normed

    @pl.when(f == 0)
    def _():
        acc[rows, :] = jnp.zeros((TM, acc.shape[1]), jnp.float32)

    for sub in range(SUB_FWD):
        size = TM // SUB_FWD
        here = pl.ds(sub * size, size)
        there = pl.ds(pl.multiple_of(m * TM + sub * size, size), size)
        normed = n_all[there, :]
        gate = jnp.dot(normed, wg_ref[...], preferred_element_type=jnp.float32)
        up = jnp.dot(normed, wu_ref[...], preferred_element_type=jnp.float32)
        gate_ref[here, :] = gate
        up_ref[here, :] = up
        act = (gate * jax.nn.sigmoid(gate) * up).astype(jnp.bfloat16)
        act_ref[here, :] = act
        acc[there, :] += jnp.dot(act, wd_ref[...], preferred_element_type=jnp.float32)

    @pl.when(f == pl.num_programs(0) - 1)
    def _():
        out_ref[...] = (h_ref[...].astype(jnp.float32) + acc[rows, :]).astype(jnp.bfloat16)


def fwd_layer(axis, hidden, wg, wu, wd, shards=()):
    tokens, width = hidden.shape
    ff = wg.shape[1]
    nf, nm = ff // TF, tokens // TM
    more = len(shards)
    result = pl.pallas_call(
        functools.partial(fwd_gather_kernel, axis) if more else fwd_kernel,
        grid=(nf, nm),
        in_specs=[
            pl.BlockSpec((TM, width), lambda f, m: (m, 0)),
            pl.BlockSpec((width, TF), lambda f, m: (0, f)),
            pl.BlockSpec((width, TF), lambda f, m: (0, f)),
            pl.BlockSpec((TF, width), lambda f, m: (f, 0)),
        ]
        + [ANY] * more,
        out_specs=[
            pl.BlockSpec((TM, width), lambda f, m: (jnp.where(f == nf - 1, m, 0), 0)),
            pl.BlockSpec((TM, width), lambda f, m: (jnp.where(f == 0, m, nm - 1), 0)),
            pl.BlockSpec((TM, TF), lambda f, m: (m, f)),
            pl.BlockSpec((TM, TF), lambda f, m: (m, f)),
            pl.BlockSpec((TM, TF), lambda f, m: (m, f)),
        ]
        + [ANY] * more,
        out_shape=[
            jax.ShapeDtypeStruct((tokens, width), jnp.bfloat16),
            jax.ShapeDtypeStruct((tokens, width), jnp.bfloat16),
            jax.ShapeDtypeStruct((tokens, ff), jnp.float32),
            jax.ShapeDtypeStruct((tokens, ff), jnp.float32),
            jax.ShapeDtypeStruct((tokens, ff), jnp.bfloat16),
        ]
        + full_shapes(shards),
        scratch_shapes=[pltpu.VMEM((tokens, width), jnp.bfloat16), pltpu.VMEM((tokens, width), jnp.float32)]
        + (GATHER_SCRATCH if more else []),
        compiler_params=pltpu.CompilerParams(
            dimension_semantics=("arbitrary", "arbitrary"),
            vmem_limit_bytes=VMEM_BYTES,
            **(dict(collective_id=1, has_side_effects=True) if more else {}),
        ),
        cost_estimate=pl.CostEstimate(flops=6 * tokens * width * ff, bytes_accessed=12 * tokens * ff, transcendentals=0),
        name="fwd_gather" if more else "fwd_layer",
    )(hidden, wg, wu, wd, *shards)
    return result[:5], flat(result[5:])


def bwd_kernel(h_ref, g_ref, gate_ref, up_ref, wg_ref, wu_ref, wd_ref, out_ref, dgate_ref, dup_ref, acc, wg_t, wu_t, wd_t):
    f, m = pl.program_id(0), pl.program_id(1)
    rows = pl.ds(pl.multiple_of(m * TM, TM), TM)

    @pl.when(m == 0)
    def _():
        wd_t[...] = wd_ref[...].T
        wg_t[...] = wg_ref[...].T
        wu_t[...] = wu_ref[...].T

    @pl.when(f == 0)
    def _():
        acc[rows, :] = jnp.zeros((TM, acc.shape[1]), jnp.float32)

    for sub in range(SUB_BWD):
        size = TM // SUB_BWD
        here = pl.ds(sub * size, size)
        there = pl.ds(pl.multiple_of(m * TM + sub * size, size), size)
        d_act = jnp.dot(g_ref[here, :], wd_t[...], preferred_element_type=jnp.float32)
        gate, up = gate_ref[here, :], up_ref[here, :]
        sig = jax.nn.sigmoid(gate)
        d_gate = (d_act * up * (sig * (1.0 + gate * (1.0 - sig)))).astype(jnp.bfloat16)
        d_up = (d_act * (gate * sig)).astype(jnp.bfloat16)
        dgate_ref[here, :] = d_gate
        dup_ref[here, :] = d_up
        acc[there, :] += jnp.dot(d_gate, wg_t[...], preferred_element_type=jnp.float32) + jnp.dot(
            d_up, wu_t[...], preferred_element_type=jnp.float32
        )

    @pl.when(f == pl.num_programs(0) - 1)
    def _():
        h_f32 = h_ref[...].astype(jnp.float32)
        inv_rms = lax.rsqrt(jnp.mean(h_f32 * h_f32, axis=-1, keepdims=True) + NORM_EPS)
        d_norm = acc[rows, :]
        d_hid = inv_rms * d_norm - h_f32 * (inv_rms * inv_rms * inv_rms) * jnp.mean(d_norm * h_f32, axis=-1, keepdims=True)
        out_ref[...] = (g_ref[...].astype(jnp.float32) + d_hid).astype(jnp.bfloat16)


def bwd_layer(hidden, grad_in, gate, up, wg, wu, wd):
    tokens, width = hidden.shape
    ff = wg.shape[1]
    nf, nm = ff // TF, tokens // TM
    return pl.pallas_call(
        bwd_kernel,
        grid=(nf, nm),
        in_specs=[
            pl.BlockSpec((TM, width), lambda f, m: (jnp.where(f == nf - 1, m, 0), 0)),
            pl.BlockSpec((TM, width), lambda f, m: (m, 0)),
            pl.BlockSpec((TM, TF), lambda f, m: (m, f)),
            pl.BlockSpec((TM, TF), lambda f, m: (m, f)),
            pl.BlockSpec((width, TF), lambda f, m: (0, f)),
            pl.BlockSpec((width, TF), lambda f, m: (0, f)),
            pl.BlockSpec((TF, width), lambda f, m: (f, 0)),
        ],
        out_specs=[
            pl.BlockSpec((TM, width), lambda f, m: (jnp.where(f == nf - 1, m, 0), 0)),
            pl.BlockSpec((TM, TF), lambda f, m: (m, f)),
            pl.BlockSpec((TM, TF), lambda f, m: (m, f)),
        ],
        out_shape=[
            jax.ShapeDtypeStruct((tokens, width), jnp.bfloat16),
            jax.ShapeDtypeStruct((tokens, ff), jnp.bfloat16),
            jax.ShapeDtypeStruct((tokens, ff), jnp.bfloat16),
        ],
        scratch_shapes=[
            pltpu.VMEM((tokens, width), jnp.float32),
            pltpu.VMEM((TF, width), jnp.bfloat16),
            pltpu.VMEM((TF, width), jnp.bfloat16),
            pltpu.VMEM((width, TF), jnp.bfloat16),
        ],
        compiler_params=params(("arbitrary", "arbitrary")),
        cost_estimate=pl.CostEstimate(flops=6 * tokens * width * ff, bytes_accessed=12 * tokens * ff, transcendentals=0),
        name="bwd_layer",
    )(hidden, grad_in, gate, up, wg, wu, wd)


def dw_in_kernel(n_ref, d_ref, out_ref):
    out_ref[...] = t_dot(n_ref[...], d_ref[...])


def dw_in(normed, d_hidden):
    tokens, width = normed.shape
    ff = d_hidden.shape[1]
    return pl.pallas_call(
        dw_in_kernel,
        grid=(ff // TD,),
        in_specs=[pl.BlockSpec((tokens, width), lambda f: (0, 0)), pl.BlockSpec((tokens, TD), lambda f: (0, f))],
        out_specs=pl.BlockSpec((width, TD), lambda f: (0, f)),
        out_shape=jax.ShapeDtypeStruct((width, ff), jnp.float32),
        compiler_params=params(("arbitrary",)),
        cost_estimate=pl.CostEstimate(flops=2 * tokens * width * ff, bytes_accessed=4 * width * ff, transcendentals=0),
        name="dw_in",
    )(normed, d_hidden)


def dw_in_split_kernel(block_of, n_ref, d_ref, keep_ref, send_ref, full):
    shard = keep_ref.shape[1]
    full[...] = t_dot(n_ref[...], d_ref[...])
    core = block_of[8]
    for q in range(8):
        base = block_of[q] * (2 * shard)
        keep_ref[q] = full[pl.ds(pl.multiple_of(base + core * shard, shard), shard), :]
        send_ref[q] = full[pl.ds(pl.multiple_of(base + (1 - core) * shard, shard), shard), :]


def dw_in_split(block_of, normed, d_hidden, first, cols):
    tokens, width = normed.shape
    tile = TD
    shard = width // 16
    out = jax.ShapeDtypeStruct((8, shard, cols), jnp.float32)
    return pl.pallas_call(
        dw_in_split_kernel,
        grid_spec=pltpu.PrefetchScalarGridSpec(
            num_scalar_prefetch=1,
            grid=(cols // tile,),
            in_specs=[
                pl.BlockSpec((tokens, width), lambda f, t: (0, 0)),
                pl.BlockSpec((tokens, tile), lambda f, t: (0, first // tile + f)),
            ],
            out_specs=[pl.BlockSpec((8, shard, tile), lambda f, t: (0, 0, f))] * 2,
            scratch_shapes=[pltpu.VMEM((width, tile), jnp.float32)],
        ),
        out_shape=[out, out],
        compiler_params=params(("arbitrary",)),
        cost_estimate=pl.CostEstimate(flops=2 * tokens * width * cols, bytes_accessed=4 * width * cols, transcendentals=0),
        name="dw_in_split",
    )(block_of, normed, d_hidden)


def dw_down_split_kernel(block_of, act_ref, g_ref, keep_ref, send_ref, full):
    shard = keep_ref.shape[1]
    full[...] = t_dot(act_ref[...], g_ref[...])
    core = block_of[8]
    keep_ref[0] = full[pl.ds(pl.multiple_of(core * shard, shard), shard), :]
    send_ref[0] = full[pl.ds(pl.multiple_of((1 - core) * shard, shard), shard), :]


def dw_down_split(block_of, act, grad_in):
    tokens, ff = act.shape
    width = grad_in.shape[1]
    shard = ff // 16
    out = jax.ShapeDtypeStruct((8, shard, width), jnp.float32)
    return pl.pallas_call(
        dw_down_split_kernel,
        grid_spec=pltpu.PrefetchScalarGridSpec(
            num_scalar_prefetch=1,
            grid=(8,),
            in_specs=[
                pl.BlockSpec((tokens, 2 * shard), lambda q, t: (0, t[q])),
                pl.BlockSpec((tokens, width), lambda q, t: (0, 0)),
            ],
            out_specs=[pl.BlockSpec((1, shard, width), lambda q, t: (q, 0, 0))] * 2,
            scratch_shapes=[pltpu.VMEM((2 * shard, width), jnp.float32)],
        ),
        out_shape=[out, out],
        compiler_params=params(("arbitrary",)),
        cost_estimate=pl.CostEstimate(flops=2 * tokens * width * ff, bytes_accessed=4 * width * ff, transcendentals=0),
        name="dw_down_split",
    )(block_of, act, grad_in)


def solution(mesh):
    group_axis = mesh.axis_names[0]
    size = mesh.shape[group_axis]
    weight_spec = P(None, group_axis, None)
    token_spec = P(group_axis)

    def swap(value, bit):
        return lax.ppermute(value, group_axis, [(i, i ^ bit) for i in range(size)])

    def chip_table(order):
        me = lax.axis_index(group_axis).astype(jnp.int32)
        entries = []
        for q in range(8):
            bits = sum(bit for i, bit in enumerate(order) if (q >> (2 - i)) & 1)
            entries.append((me ^ bits) >> 1)
        return jnp.stack(entries + [me & 1])

    def fence(value, anchors):
        return lax.optimization_barrier((value,) + tuple(anchors))[0]

    class Chain:
        def __init__(self, keep, send, order, now):
            self.keep, self.bits, self.got = keep, (CORE,) + order, []
            self.result = None
            self.unit = FLIGHT * keep.size / (8 * 64 * 3072)
            self.launch(send, now)

        def launch(self, part, now):
            stage = len(self.got)
            self.flying = swap(part, self.bits[stage])
            self.ready = now + 2.0 + self.unit * (0.15, 1.0, 0.5, 0.25)[stage]

        def step(self, anchors, now):
            self.got.append(fence(self.flying, anchors))
            low, high = ((4, 8), (2, 4), (1, 2), (0, 1))[len(self.got) - 1]
            total = self.keep[low:high]
            for arrived in self.got:
                total = total + arrived[low:high]
            if low == 0:
                self.result, self.ready = total[0], None
            else:
                self.launch(total, now)
            return total

    def local_step(h_in, w_gate, w_up, w_down, grad_out):
        stacks = (w_gate, w_up, w_down)
        num_layers = w_gate.shape[0]
        shape = h_in.shape
        hidden = h_in.reshape(-1, shape[-1])
        grad_in = grad_out.reshape(-1, shape[-1])
        shards = [tuple(w[layer] for w in stacks) for layer in range(num_layers)]
        saved = []
        weights = gather_first(group_axis, shards[0])
        for layer in range(num_layers):
            following = shards[layer + 1] if layer + 1 < num_layers else ()
            (out, normed, gate, up, act), gathered = fwd_layer(group_axis, hidden, *weights, following)
            saved.append((hidden, normed, gate, up, act, weights))
            hidden, weights = out, gathered
        h_out = hidden

        clock = 0.0
        chains = []
        parts = []

        def slot(anchor, spent):
            nonlocal clock, parts
            clock += spent
            parts = [c.step([anchor], clock) for c in chains if c.ready is not None and c.ready <= clock]

        downs, ups, gates = {}, {}, {}
        for layer in reversed(range(num_layers)):
            hidden, normed, gate, up, act, weights = saved[layer]
            orders = [tuple(AXIS_BITS[(layer + j + i) % 3] for i in range(3)) for j in range(3)]
            keep, send = dw_down_split(chip_table(orders[0]), act, fence(grad_in, parts))
            slot(keep, T_DOWN)
            downs[layer] = Chain(keep, send, orders[0], clock)
            chains.append(downs[layer])
            grad_new, d_gate, d_up = bwd_layer(hidden, fence(grad_in, [keep] + parts), gate, up, *weights)
            slot(d_up, T_BWD)
            d_up = fence(d_up, parts)
            full_up = dw_in(normed, d_up)
            ups[layer] = lax.psum_scatter(full_up, group_axis, scatter_dimension=0, tiled=True)
            slot(full_up, T_IN)
            d_gate = fence(d_gate, [full_up] + parts)
            ff = d_gate.shape[1]
            pieces = 3 if layer == 0 else 1
            gates[layer] = []
            for j in range(pieces):
                order = orders[(1 + j) % 3]
                table, cols = chip_table(order), ff // pieces
                keep, send = dw_in_split(table, normed, d_gate, j * cols, cols)
                slot(keep, T_IN / pieces)
                gates[layer].append(Chain(keep, send, order, clock))
                chains.append(gates[layer][-1])
                d_gate = fence(d_gate, [keep] + parts)
            grad_in = fence(grad_new, [keep] + parts)

        while any(c.ready is not None for c in chains):
            first = min((c for c in chains if c.ready is not None), key=lambda c: c.ready)
            clock = max(clock, first.ready)
            first.step([], clock)
        layers = range(num_layers)
        dw_gate = jnp.stack([jnp.concatenate([c.result for c in gates[i]], axis=-1) for i in layers])
        dw_up = jnp.stack([ups[i] for i in layers])
        dw_down = jnp.stack([downs[i].result for i in layers])
        return h_out.reshape(shape), grad_in.reshape(shape), dw_gate, dw_up, dw_down

    return jax.shard_map(
        local_step,
        mesh=mesh,
        in_specs=(token_spec, weight_spec, weight_spec, weight_spec, token_spec),
        out_specs=(token_spec, token_spec, weight_spec, weight_spec, weight_spec),
        check_vma=False,
    )
```

```python
import functools

import jax
import jax.numpy as jnp
from jax import lax
from jax.experimental import pallas as pl
from jax.experimental.pallas import tpu as pltpu
from jax.sharding import PartitionSpec as P


NORM_EPS = 1e-5
CORE, X, Y, Z = 1, 2, 4, 8
AXIS_BITS = (X, Y, Z)
TM = 1024
TF = 768
SUB_FWD, SUB_BWD = 2, 2
TH = 512
TD = 512
VMEM_BYTES = 60 * 1024 * 1024
FLIGHT, T_DOWN, T_HID, T_IN, T_OUT = 85.0, 21.0, 33.0, 20.0, 35.0


def params(semantics):
    return pltpu.CompilerParams(dimension_semantics=semantics, vmem_limit_bytes=VMEM_BYTES)


def dot_t(lhs, rhs):
    return lax.dot_general(lhs, rhs, (((1,), (1,)), ((), ())), preferred_element_type=jnp.float32)


def t_dot(lhs, rhs):
    return lax.dot_general(lhs, rhs, (((0,), (0,)), ((), ())), preferred_element_type=jnp.float32)


MESH_ID = pl.DeviceIdType.MESH
GATHER_STEPS = (0, 2, 5, 7)


class Gather:
    def __init__(self, axis, shards, fulls, sends, recvs, locals_):
        self.shards, self.fulls = shards, fulls
        self.sends, self.recvs, self.locals_ = sends, recvs, locals_
        me = lax.axis_index(axis)
        self.core = me % 2
        self.coord = {Z: me // 8, Y: (me // 4) % 2, X: (me // 2) % 2}
        self.partner = {
            CORE: me + 1 - 2 * self.core,
            X: me + 2 - 4 * self.coord[X],
            Y: me + 4 - 8 * self.coord[Y],
            Z: me + 8 - 16 * self.coord[Z],
        }

    def order(self, k):
        return tuple(AXIS_BITS[(k + i) % 3] for i in range(3))

    def piece(self, k, free=(), flipped=None):
        index = []
        for bit in (Z, Y, X):
            if bit in free:
                index.append(slice(None))
            elif bit == flipped:
                index.append(1 - self.coord[bit])
            else:
                index.append(self.coord[bit])
        return self.fulls[k].at[tuple(index) + (self.core,)]

    def remote(self, k, slot, src, dst, bit):
        return pltpu.make_async_remote_copy(
            src_ref=src,
            dst_ref=dst,
            send_sem=self.sends.at[k, slot],
            recv_sem=self.recvs.at[k, slot],
            device_id=(self.partner[bit],),
            device_id_type=MESH_ID,
        )

    def along(self, k, s, j):
        if j == 0:
            return self.remote(k, (0, 1, 3)[s], self.shards[k], self.piece(k), self.order(k)[s])
        part = self.piece(k, self.order(k)[: j - 1], self.order(k)[j - 1])
        return self.remote(k, (0, 1, 3)[s] + j, part, part, self.order(k)[s])

    def arrived(self, k, s, j):
        return self.along(k, s, j)

    def across(self, k, s, j):
        if s < 0:
            return self.remote(k, 6, self.shards[k], self.piece(k), CORE)
        order = self.order(k)
        free = order[: j - 1] if j > 0 else ()
        index = []
        for bit in (Z, Y, X):
            if bit in free:
                index.append(slice(None))
            elif bit == order[s] or (j > 0 and bit == order[j - 1]):
                index.append(1 - self.coord[bit])
            else:
                index.append(self.coord[bit])
        part = self.fulls[k].at[tuple(index) + (self.core,)]
        return self.remote(k, 7 + (0, 1, 3)[s] + j, part, part, CORE)

    def own(self, k):
        return pltpu.make_async_copy(self.shards[k], self.piece(k), self.locals_.at[k])

    def begin(self):
        barrier = pltpu.get_barrier_semaphore()
        for bit in (CORE, X, Y, Z):
            pl.semaphore_signal(barrier, inc=1, device_id=(self.partner[bit],), device_id_type=MESH_ID)
        pl.semaphore_wait(barrier, 4)
        for s in range(3):
            for k in range(3):
                self.along(k, s, 0).start()
        for k in range(3):
            self.across(k, -1, 0).start()
            self.own(k).start()

    def take(self, k, s, j):
        self.arrived(k, s, j).wait_recv()
        self.across(k, s, j).start()

    def advance(self, s):
        for k in range(3):
            if s == 1:
                self.take(k, 0, 0)
                self.along(k, 1, 1).start()
                self.along(k, 2, 1).start()
            elif s == 2:
                self.take(k, 1, 0)
                self.take(k, 1, 1)
                self.along(k, 2, 2).start()
            else:
                self.take(k, 2, 0)
                self.take(k, 2, 1)

    def finish(self):
        for k in range(3):
            self.take(k, 2, 2)
        for k in range(3):
            self.own(k).wait()
            for s in range(3):
                for j in range(s + 1):
                    self.along(k, s, j).wait_send()
                    self.across(k, s, j).wait()
            self.across(k, -1, 0).wait()


GATHER_SCRATCH = [
    pltpu.SemaphoreType.DMA((3, 13)),
    pltpu.SemaphoreType.DMA((3, 13)),
    pltpu.SemaphoreType.DMA((3,)),
]
ANY = pl.BlockSpec(memory_space=pl.ANY)


def full_shapes(shards):
    return [jax.ShapeDtypeStruct((2, 2, 2, 2) + w.shape, w.dtype) for w in shards]


def flat(fulls):
    return tuple(w.reshape(-1, w.shape[-1]) for w in fulls)


def gather_first(axis, shards):
    def kernel(*refs):
        gather = Gather(axis, refs[:3], refs[3:6], *refs[6:9])
        gather.begin()
        for s in (1, 2, 3):
            gather.advance(s)
        gather.finish()

    return flat(
        pl.pallas_call(
            kernel,
            in_specs=[ANY] * 3,
            out_specs=[ANY] * 3,
            out_shape=full_shapes(shards),
            scratch_shapes=GATHER_SCRATCH,
            compiler_params=pltpu.CompilerParams(collective_id=0, has_side_effects=True),
            name="gather_first",
        )(*shards)
    )


def fwd_gather_kernel(axis, *refs):
    main, shards, outs, fulls, scratch, sems = refs[:4], refs[4:7], refs[7:12], refs[12:15], refs[15:17], refs[17:]
    step = pl.program_id(0) * pl.num_programs(1) + pl.program_id(1)
    gather = Gather(axis, shards, fulls, *sems)
    pl.when(step == GATHER_STEPS[0])(gather.begin)
    for s in (1, 2, 3):
        pl.when(step == GATHER_STEPS[s])(functools.partial(gather.advance, s))
    fwd_kernel(*main, *outs, *scratch)
    pl.when(step == pl.num_programs(0) * pl.num_programs(1) - 1)(gather.finish)


def fwd_kernel(h_ref, wg_ref, wu_ref, wd_ref, out_ref, n_ref, gate_ref, up_ref, act_ref, n_all, acc):
    f, m = pl.program_id(0), pl.program_id(1)
    rows = pl.ds(pl.multiple_of(m * TM, TM), TM)

    @pl.when(f == 0)
    def _():
        h_f32 = h_ref[...].astype(jnp.float32)
        inv_rms = lax.rsqrt(jnp.mean(h_f32 * h_f32, axis=-1, keepdims=True) + NORM_EPS)
        normed = (h_f32 * inv_rms).astype(jnp.bfloat16)
        n_all[rows, :] = normed
        n_ref[...] = normed

    @pl.when(f == 0)
    def _():
        acc[rows, :] = jnp.zeros((TM, acc.shape[1]), jnp.float32)

    for sub in range(SUB_FWD):
        size = TM // SUB_FWD
        here = pl.ds(sub * size, size)
        there = pl.ds(pl.multiple_of(m * TM + sub * size, size), size)
        normed = n_all[there, :]
        gate = jnp.dot(normed, wg_ref[...], preferred_element_type=jnp.float32)
        up = jnp.dot(normed, wu_ref[...], preferred_element_type=jnp.float32)
        gate_ref[here, :] = gate
        up_ref[here, :] = up
        act = (gate * jax.nn.sigmoid(gate) * up).astype(jnp.bfloat16)
        act_ref[here, :] = act
        acc[there, :] += jnp.dot(act, wd_ref[...], preferred_element_type=jnp.float32)

    @pl.when(f == pl.num_programs(0) - 1)
    def _():
        out_ref[...] = (h_ref[...].astype(jnp.float32) + acc[rows, :]).astype(jnp.bfloat16)


def fwd_layer(axis, hidden, wg, wu, wd, shards=()):
    tokens, width = hidden.shape
    ff = wg.shape[1]
    nf, nm = ff // TF, tokens // TM
    more = len(shards)
    result = pl.pallas_call(
        functools.partial(fwd_gather_kernel, axis) if more else fwd_kernel,
        grid=(nf, nm),
        in_specs=[
            pl.BlockSpec((TM, width), lambda f, m: (m, 0)),
            pl.BlockSpec((width, TF), lambda f, m: (0, f)),
            pl.BlockSpec((width, TF), lambda f, m: (0, f)),
            pl.BlockSpec((TF, width), lambda f, m: (f, 0)),
        ]
        + [ANY] * more,
        out_specs=[
            pl.BlockSpec((TM, width), lambda f, m: (jnp.where(f == nf - 1, m, 0), 0)),
            pl.BlockSpec((TM, width), lambda f, m: (jnp.where(f == 0, m, nm - 1), 0)),
            pl.BlockSpec((TM, TF), lambda f, m: (m, f)),
            pl.BlockSpec((TM, TF), lambda f, m: (m, f)),
            pl.BlockSpec((TM, TF), lambda f, m: (m, f)),
        ]
        + [ANY] * more,
        out_shape=[
            jax.ShapeDtypeStruct((tokens, width), jnp.bfloat16),
            jax.ShapeDtypeStruct((tokens, width), jnp.bfloat16),
            jax.ShapeDtypeStruct((tokens, ff), jnp.float32),
            jax.ShapeDtypeStruct((tokens, ff), jnp.float32),
            jax.ShapeDtypeStruct((tokens, ff), jnp.bfloat16),
        ]
        + full_shapes(shards),
        scratch_shapes=[pltpu.VMEM((tokens, width), jnp.bfloat16), pltpu.VMEM((tokens, width), jnp.float32)]
        + (GATHER_SCRATCH if more else []),
        compiler_params=pltpu.CompilerParams(
            dimension_semantics=("arbitrary", "arbitrary"),
            vmem_limit_bytes=VMEM_BYTES,
            **(dict(collective_id=1, has_side_effects=True) if more else {}),
        ),
        cost_estimate=pl.CostEstimate(flops=6 * tokens * width * ff, bytes_accessed=12 * tokens * ff, transcendentals=0),
        name="fwd_gather" if more else "fwd_layer",
    )(hidden, wg, wu, wd, *shards)
    return result[:5], flat(result[5:])


def hidden_grad_kernel(g_ref, gate_ref, up_ref, wd_ref, dgate_ref, dup_ref):
    m = pl.program_id(1)
    size = TH // SUB_BWD
    for sub in range(SUB_BWD):
        here = pl.ds(sub * size, size)
        there = pl.ds(pl.multiple_of(m * TH + sub * size, size), size)
        d_act = dot_t(g_ref[there, :], wd_ref[...])
        gate, up = gate_ref[here, :], up_ref[here, :]
        sig = jax.nn.sigmoid(gate)
        dgate_ref[here, :] = (d_act * up * (sig * (1.0 + gate * (1.0 - sig)))).astype(jnp.bfloat16)
        dup_ref[here, :] = (d_act * (gate * sig)).astype(jnp.bfloat16)


def hidden_grad(grad_in, gate, up, wd):
    tokens, width = grad_in.shape
    ff = wd.shape[0]
    tile = pl.BlockSpec((TH, TF), lambda f, m: (m, f))
    out = jax.ShapeDtypeStruct((tokens, ff), jnp.bfloat16)
    return pl.pallas_call(
        hidden_grad_kernel,
        grid=(ff // TF, tokens // TH),
        in_specs=[
            pl.BlockSpec((tokens, width), lambda f, m: (0, 0)),
            tile,
            tile,
            pl.BlockSpec((TF, width), lambda f, m: (f, 0)),
        ],
        out_specs=[tile, tile],
        out_shape=[out, out],
        compiler_params=params(("arbitrary", "arbitrary")),
        cost_estimate=pl.CostEstimate(flops=2 * tokens * width * ff, bytes_accessed=12 * tokens * ff, transcendentals=0),
        name="hidden_grad",
    )(grad_in, gate, up, wd)


def input_grad_kernel(h_ref, g_ref, dgate_ref, dup_ref, wg_ref, wu_ref, out_ref, acc):
    f, m = pl.program_id(0), pl.program_id(1)
    rows = pl.ds(pl.multiple_of(m * TM, TM), TM)
    part = dot_t(dgate_ref[...], wg_ref[...]) + dot_t(dup_ref[...], wu_ref[...])

    @pl.when(f == 0)
    def _():
        acc[rows, :] = part

    @pl.when(f > 0)
    def _():
        acc[rows, :] += part

    @pl.when(f == pl.num_programs(0) - 1)
    def _():
        h_f32 = h_ref[...].astype(jnp.float32)
        inv_rms = lax.rsqrt(jnp.mean(h_f32 * h_f32, axis=-1, keepdims=True) + NORM_EPS)
        d_norm = acc[rows, :]
        d_hid = inv_rms * d_norm - h_f32 * (inv_rms * inv_rms * inv_rms) * jnp.mean(d_norm * h_f32, axis=-1, keepdims=True)
        out_ref[...] = (g_ref[...].astype(jnp.float32) + d_hid).astype(jnp.bfloat16)


def input_grad(hidden, grad_in, d_gate, d_up, wg, wu):
    tokens, width = hidden.shape
    ff = wg.shape[1]
    nf = ff // TF
    late = pl.BlockSpec((TM, width), lambda f, m: (jnp.where(f == nf - 1, m, 0), 0))
    return pl.pallas_call(
        input_grad_kernel,
        grid=(nf, tokens // TM),
        in_specs=[
            late,
            late,
            pl.BlockSpec((TM, TF), lambda f, m: (m, f)),
            pl.BlockSpec((TM, TF), lambda f, m: (m, f)),
            pl.BlockSpec((width, TF), lambda f, m: (0, f)),
            pl.BlockSpec((width, TF), lambda f, m: (0, f)),
        ],
        out_specs=late,
        out_shape=jax.ShapeDtypeStruct((tokens, width), jnp.bfloat16),
        scratch_shapes=[pltpu.VMEM((tokens, width), jnp.float32)],
        compiler_params=params(("arbitrary", "arbitrary")),
        cost_estimate=pl.CostEstimate(flops=4 * tokens * width * ff, bytes_accessed=8 * tokens * ff, transcendentals=0),
        name="input_grad",
    )(hidden, grad_in, d_gate, d_up, wg, wu)


def dw_in_kernel(n_ref, d_ref, out_ref):
    out_ref[...] = t_dot(n_ref[...], d_ref[...])


def dw_in(normed, d_hidden):
    tokens, width = normed.shape
    ff = d_hidden.shape[1]
    return pl.pallas_call(
        dw_in_kernel,
        grid=(ff // TD,),
        in_specs=[pl.BlockSpec((tokens, width), lambda f: (0, 0)), pl.BlockSpec((tokens, TD), lambda f: (0, f))],
        out_specs=pl.BlockSpec((width, TD), lambda f: (0, f)),
        out_shape=jax.ShapeDtypeStruct((width, ff), jnp.float32),
        compiler_params=params(("arbitrary",)),
        cost_estimate=pl.CostEstimate(flops=2 * tokens * width * ff, bytes_accessed=4 * width * ff, transcendentals=0),
        name="dw_in",
    )(normed, d_hidden)


def dw_in_split_kernel(block_of, n_ref, d_ref, keep_ref, send_ref, full):
    shard = keep_ref.shape[1]
    full[...] = t_dot(n_ref[...], d_ref[...])
    core = block_of[8]
    for q in range(8):
        base = block_of[q] * (2 * shard)
        keep_ref[q] = full[pl.ds(pl.multiple_of(base + core * shard, shard), shard), :]
        send_ref[q] = full[pl.ds(pl.multiple_of(base + (1 - core) * shard, shard), shard), :]


def dw_in_split(block_of, normed, d_hidden, first, cols):
    tokens, width = normed.shape
    tile = TD
    shard = width // 16
    out = jax.ShapeDtypeStruct((8, shard, cols), jnp.float32)
    return pl.pallas_call(
        dw_in_split_kernel,
        grid_spec=pltpu.PrefetchScalarGridSpec(
            num_scalar_prefetch=1,
            grid=(cols // tile,),
            in_specs=[
                pl.BlockSpec((tokens, width), lambda f, t: (0, 0)),
                pl.BlockSpec((tokens, tile), lambda f, t: (0, first // tile + f)),
            ],
            out_specs=[pl.BlockSpec((8, shard, tile), lambda f, t: (0, 0, f))] * 2,
            scratch_shapes=[pltpu.VMEM((width, tile), jnp.float32)],
        ),
        out_shape=[out, out],
        compiler_params=params(("arbitrary",)),
        cost_estimate=pl.CostEstimate(flops=2 * tokens * width * cols, bytes_accessed=4 * width * cols, transcendentals=0),
        name="dw_in_split",
    )(block_of, normed, d_hidden)


def dw_down_split_kernel(block_of, act_ref, g_ref, keep_ref, send_ref, full):
    shard = keep_ref.shape[1]
    full[...] = t_dot(act_ref[...], g_ref[...])
    core = block_of[8]
    keep_ref[0] = full[pl.ds(pl.multiple_of(core * shard, shard), shard), :]
    send_ref[0] = full[pl.ds(pl.multiple_of((1 - core) * shard, shard), shard), :]


def dw_down_split(block_of, act, grad_in):
    tokens, ff = act.shape
    width = grad_in.shape[1]
    shard = ff // 16
    out = jax.ShapeDtypeStruct((8, shard, width), jnp.float32)
    return pl.pallas_call(
        dw_down_split_kernel,
        grid_spec=pltpu.PrefetchScalarGridSpec(
            num_scalar_prefetch=1,
            grid=(8,),
            in_specs=[
                pl.BlockSpec((tokens, 2 * shard), lambda q, t: (0, t[q])),
                pl.BlockSpec((tokens, width), lambda q, t: (0, 0)),
            ],
            out_specs=[pl.BlockSpec((1, shard, width), lambda q, t: (q, 0, 0))] * 2,
            scratch_shapes=[pltpu.VMEM((2 * shard, width), jnp.float32)],
        ),
        out_shape=[out, out],
        compiler_params=params(("arbitrary",)),
        cost_estimate=pl.CostEstimate(flops=2 * tokens * width * ff, bytes_accessed=4 * width * ff, transcendentals=0),
        name="dw_down_split",
    )(block_of, act, grad_in)


def solution(mesh):
    group_axis = mesh.axis_names[0]
    size = mesh.shape[group_axis]
    weight_spec = P(None, group_axis, None)
    token_spec = P(group_axis)

    def swap(value, bit):
        return lax.ppermute(value, group_axis, [(i, i ^ bit) for i in range(size)])

    def chip_table(order):
        me = lax.axis_index(group_axis).astype(jnp.int32)
        entries = []
        for q in range(8):
            bits = sum(bit for i, bit in enumerate(order) if (q >> (2 - i)) & 1)
            entries.append((me ^ bits) >> 1)
        return jnp.stack(entries + [me & 1])

    def fence(value, anchors):
        return lax.optimization_barrier((value,) + tuple(anchors))[0]

    class Chain:
        def __init__(self, keep, send, order, now):
            self.keep, self.bits, self.got = keep, (CORE,) + order, []
            self.result = None
            self.unit = FLIGHT * keep.size / (8 * 64 * 3072)
            self.launch(send, now)

        def launch(self, part, now):
            stage = len(self.got)
            self.flying = swap(part, self.bits[stage])
            self.ready = now + 2.0 + self.unit * (0.15, 1.0, 0.5, 0.25)[stage]

        def step(self, anchors, now):
            self.got.append(fence(self.flying, anchors))
            low, high = ((4, 8), (2, 4), (1, 2), (0, 1))[len(self.got) - 1]
            total = self.keep[low:high]
            for arrived in self.got:
                total = total + arrived[low:high]
            if low == 0:
                self.result, self.ready = total[0], None
            else:
                self.launch(total, now)
            return total

    def local_step(h_in, w_gate, w_up, w_down, grad_out):
        stacks = (w_gate, w_up, w_down)
        num_layers = w_gate.shape[0]
        shape = h_in.shape
        hidden = h_in.reshape(-1, shape[-1])
        grad_in = grad_out.reshape(-1, shape[-1])
        shards = [tuple(w[layer] for w in stacks) for layer in range(num_layers)]
        saved = []
        weights = gather_first(group_axis, shards[0])
        for layer in range(num_layers):
            following = shards[layer + 1] if layer + 1 < num_layers else ()
            (out, normed, gate, up, act), gathered = fwd_layer(group_axis, hidden, *weights, following)
            saved.append((hidden, normed, gate, up, act, weights))
            hidden, weights = out, gathered
        h_out = hidden

        clock = 0.0
        chains = []
        parts = []

        def slot(anchor, spent):
            nonlocal clock, parts
            clock += spent
            parts = [c.step([anchor], clock) for c in chains if c.ready is not None and c.ready <= clock]

        downs, ups, gates = {}, {}, {}
        for layer in reversed(range(num_layers)):
            hidden, normed, gate, up, act, weights = saved[layer]
            orders = [tuple(AXIS_BITS[(layer + j + i) % 3] for i in range(3)) for j in range(3)]
            keep, send = dw_down_split(chip_table(orders[0]), act, fence(grad_in, parts))
            slot(keep, T_DOWN)
            downs[layer] = Chain(keep, send, orders[0], clock)
            chains.append(downs[layer])
            d_gate, d_up = hidden_grad(fence(grad_in, [keep] + parts), gate, up, weights[2])
            slot(d_up, T_HID)
            d_up = fence(d_up, parts)
            full_up = dw_in(normed, d_up)
            ups[layer] = lax.psum_scatter(full_up, group_axis, scatter_dimension=0, tiled=True)
            slot(full_up, T_IN)
            d_gate = fence(d_gate, [full_up] + parts)
            ff = d_gate.shape[1]
            pieces = 3 if layer == 0 else 1
            gates[layer] = []
            for j in range(pieces):
                order = orders[(1 + j) % 3]
                table, cols = chip_table(order), ff // pieces
                keep, send = dw_in_split(table, normed, d_gate, j * cols, cols)
                slot(keep, T_IN / pieces)
                gates[layer].append(Chain(keep, send, order, clock))
                chains.append(gates[layer][-1])
                d_gate = fence(d_gate, [keep] + parts)
            grad_in = input_grad(hidden, grad_in, d_gate, d_up, *weights[:2])
            slot(grad_in, T_OUT)

        while any(c.ready is not None for c in chains):
            first = min((c for c in chains if c.ready is not None), key=lambda c: c.ready)
            clock = max(clock, first.ready)
            first.step([], clock)
        layers = range(num_layers)
        dw_gate = jnp.stack([jnp.concatenate([c.result for c in gates[i]], axis=-1) for i in layers])
        dw_up = jnp.stack([ups[i] for i in layers])
        dw_down = jnp.stack([downs[i].result for i in layers])
        return h_out.reshape(shape), grad_in.reshape(shape), dw_gate, dw_up, dw_down

    return jax.shard_map(
        local_step,
        mesh=mesh,
        in_specs=(token_spec, weight_spec, weight_spec, weight_spec, token_spec),
        out_specs=(token_spec, token_spec, weight_spec, weight_spec, weight_spec),
        check_vma=False,
    )
```
